32 devices in a mesh: rep: 1 (over z), data: 4 (over y), expert: 8 (over x, core).
Axes of the slice: x: 4, y: 4, z: 1, core: 2. Of those that a mesh axis runs over, the one named last changes fastest.
The devices are a block of a 4x4x8 slice.
Arguments:
- x_tok: bfloat16 [24576, 1792], P(('rep', 'expert', 'data'))
- expert_idx: int32 [24576, 8], P(('rep', 'expert', 'data'))
- gate_val: float32 [24576, 8], P(('rep', 'expert', 'data'))
- w_gate: bfloat16 [256, 1792, 512], P('expert', 'data')
- w_up: bfloat16 [256, 1792, 512], P('expert', 'data')
- w_down: bfloat16 [256, 512, 1792], P('expert', None, 'data')
- ws_gate: bfloat16 [1792, 512], P(('expert', 'data'))
- ws_up: bfloat16 [1792, 512], P(('expert', 'data'))
- ws_down: bfloat16 [512, 1792], P(None, ('expert', 'data'))
Outputs:
- output: bfloat16 [24576, 1792], P(('rep', 'expert', 'data'))
All inputs are finite; a program needn't handle non-finite values.
Results may differ from the reference program's by a relative error of at most 0.001.
Values are sent between devices in bfloat16 or wider.
A program may use at most 768 MiB of HBM per device.

```python
import jax
import jax.numpy as jnp
from jax import lax

D_MODEL = 1792
FF_EXP = 512
EXPERTS = 256
TOP = 8
FF_SHARED = 512
TOKENS_DEV = 768
BLOCKS = 32
CAPACITY = 32

TOKENS = BLOCKS * TOKENS_DEV
PAIRS = TOKENS_DEV * TOP


def draw_routing(key):
    key_score, key_bias, key_hot = jax.random.split(key, 3)
    scores = jax.random.randint(key_score, (BLOCKS, TOKENS_DEV, EXPERTS), 0, 1024, jnp.int32)
    exp_bias = jax.random.randint(key_bias, (BLOCKS, 1, EXPERTS), 0, 512, jnp.int32)
    hot_expert = jax.random.randint(key_hot, (BLOCKS, 1, 1), 0, EXPERTS, jnp.int32)
    forced = (jnp.arange(TOKENS_DEV, dtype=jnp.int32)[None, :, None] < CAPACITY) & (jnp.arange(EXPERTS, dtype=jnp.int32)[None, None, :] == hot_expert)
    ranked = (scores + exp_bias + jnp.where(forced, 4096, 0)) * EXPERTS + jnp.arange(EXPERTS, dtype=jnp.int32)
    chosen = lax.top_k(ranked, TOP)[1]
    return chosen.reshape(TOKENS, TOP).astype(jnp.int32)


def setup_inputs(seed: int = 0, part: int = 0) -> dict:
    weight_keys = jax.random.split(jax.random.key(seed), 6)
    key_x, key_route, key_gate = jax.random.split(jax.random.fold_in(jax.random.key(seed + 1), part), 3)
    scale_model = D_MODEL ** -0.5
    scale_exp = FF_EXP ** -0.5
    scale_shared = FF_SHARED ** -0.5
    x_tok = jax.random.normal(key_x, (TOKENS, D_MODEL), jnp.float32)
    gate_val = jax.random.uniform(key_gate, (TOKENS, TOP), jnp.float32, 0.2, 0.8)
    w_gate = jax.random.normal(weight_keys[0], (EXPERTS, D_MODEL, FF_EXP), jnp.float32) * scale_model
    w_up = jax.random.normal(weight_keys[1], (EXPERTS, D_MODEL, FF_EXP), jnp.float32) * scale_model
    w_down = jax.random.normal(weight_keys[2], (EXPERTS, FF_EXP, D_MODEL), jnp.float32) * scale_exp
    ws_gate = jax.random.normal(weight_keys[3], (D_MODEL, FF_SHARED), jnp.float32) * scale_model
    ws_up = jax.random.normal(weight_keys[4], (D_MODEL, FF_SHARED), jnp.float32) * scale_model
    ws_down = jax.random.normal(weight_keys[5], (FF_SHARED, D_MODEL), jnp.float32) * scale_shared
    return {"x_tok": x_tok.astype(jnp.bfloat16), "expert_idx": draw_routing(key_route), "gate_val": gate_val, "w_gate": w_gate.astype(jnp.bfloat16), "w_up": w_up.astype(jnp.bfloat16), "w_down": w_down.astype(jnp.bfloat16), "ws_gate": ws_gate.astype(jnp.bfloat16), "ws_up": ws_up.astype(jnp.bfloat16), "ws_down": ws_down.astype(jnp.bfloat16)}


def slot_block(flat_idx):
    onehot = (flat_idx[:, None] == jnp.arange(EXPERTS, dtype=jnp.int32)[None, :]).astype(jnp.int32)
    slot_idx = jnp.sum((jnp.cumsum(onehot, axis=0) - onehot) * onehot, axis=1)
    return jnp.where(slot_idx < CAPACITY, flat_idx * CAPACITY + slot_idx, EXPERTS * CAPACITY)


def source_block(dest_pos):
    return jnp.full((EXPERTS * CAPACITY,), PAIRS, jnp.int32).at[dest_pos].set(jnp.arange(PAIRS, dtype=jnp.int32), mode="drop")


def expert_ffn(tok_rows, w_gate, w_up, w_down):
    gate_pre = jnp.dot(tok_rows, w_gate, preferred_element_type=jnp.float32)
    up_pre = jnp.dot(tok_rows, w_up, preferred_element_type=jnp.float32)
    hidden = (jax.nn.silu(gate_pre) * up_pre).astype(jnp.bfloat16)
    return jnp.dot(hidden, w_down, preferred_element_type=jnp.float32).astype(jnp.bfloat16)


def reference(x_tok, expert_idx, gate_val, w_gate, w_up, w_down, ws_gate, ws_up, ws_down):
    dest_pos = jax.vmap(slot_block)(expert_idx.reshape(BLOCKS, PAIRS))
    src_pair = jax.vmap(source_block)(dest_pos)
    filled = src_pair < PAIRS
    glob_pair = jnp.minimum(src_pair, PAIRS - 1) + PAIRS * jnp.arange(BLOCKS, dtype=jnp.int32)[:, None]
    slot_gate = jnp.where(filled, gate_val.reshape(BLOCKS * PAIRS)[glob_pair], 0.0)

    def by_expert(id_table):
        return id_table.reshape(BLOCKS, EXPERTS, CAPACITY).transpose(1, 0, 2).reshape(EXPERTS, BLOCKS * CAPACITY)

    def expert_step(routed, per_expert):
        wg_e, wu_e, wd_e, tok_ids, fill_e, gate_e = per_expert
        tok_rows = jnp.where(fill_e[:, None], x_tok[tok_ids], jnp.zeros((), x_tok.dtype))
        out_rows = expert_ffn(tok_rows, wg_e, wu_e, wd_e)
        return routed.at[tok_ids].add(gate_e[:, None] * out_rows.astype(jnp.float32)), None

    routed = lax.scan(expert_step, jnp.zeros((TOKENS, D_MODEL), jnp.float32), (w_gate, w_up, w_down, by_expert(glob_pair // TOP), by_expert(filled), by_expert(slot_gate)))[0]

    def shared_of(x_blk):
        gate_pre = jnp.dot(x_blk, ws_gate, preferred_element_type=jnp.float32)
        up_pre = jnp.dot(x_blk, ws_up, preferred_element_type=jnp.float32)
        hidden = (jax.nn.silu(gate_pre) * up_pre).astype(jnp.bfloat16)
        return jnp.dot(hidden, ws_down, preferred_element_type=jnp.float32)

    shared = lax.map(shared_of, x_tok.reshape(BLOCKS, TOKENS_DEV, D_MODEL)).reshape(TOKENS, D_MODEL)
    return (x_tok.astype(jnp.float32) + shared + routed).astype(jnp.bfloat16)
```

```python
import functools

import jax
import jax.numpy as jnp
from jax import lax
from jax.experimental import pallas as pl
from jax.experimental.pallas import tpu as pltpu
from jax.sharding import PartitionSpec as P

CAP_NUM = 5
CAP_DEN = 4
LANES = 128
BF16 = jnp.bfloat16
F32 = jnp.float32


def capacity_of(tok_count, top_count, n_exp):
    return max(8, ((CAP_NUM * top_count * tok_count) // (CAP_DEN * n_exp) + 7) // 8 * 8)


def hidden_kernel(n_blk, cap, slot_ref, x_ref, wg_ref, wu_ref, h_ref, rows):
    step = pl.program_id(0)
    n_own, tok = slot_ref.shape[1:]

    @pl.when(step < n_blk)
    def _():
        slot = slot_ref[0]
        cid = lax.broadcasted_iota(jnp.int32, (cap, tok), 0)
        pick = jnp.concatenate([jnp.where(slot[e : e + 1, :] == cid, 1.0, 0.0).astype(BF16) for e in range(n_own)], axis=0)
        got = jnp.dot(pick, x_ref[0], preferred_element_type=F32).astype(BF16)
        at = pl.ds(pl.multiple_of(step * cap, cap), cap)
        for e in range(n_own):
            rows[e, at, :] = got[e * cap : (e + 1) * cap, :]

    @pl.when(step >= n_blk)
    def _():
        tok_rows = rows[step - n_blk]
        gate_pre = jnp.dot(tok_rows, wg_ref[0], preferred_element_type=F32)
        up_pre = jnp.dot(tok_rows, wu_ref[0], preferred_element_type=F32)
        h_ref[0] = (jax.nn.silu(gate_pre) * up_pre).astype(BF16)


def hidden_chunk(y, n_data, cap, slot_own, x_all, wg, wu):
    n_own, d_model, ff = wg.shape
    tok = x_all.shape[1]
    n_blk = x_all.shape[0] // n_data
    m = n_blk * cap
    blk = lambda s: jnp.minimum(s, n_blk - 1) * n_data + y
    exp = lambda s: jnp.maximum(s - n_blk, 0)
    flops = 2 * n_blk * n_own * cap * tok * d_model + 4 * m * n_own * d_model * ff
    return pl.pallas_call(
        functools.partial(hidden_kernel, n_blk, cap),
        grid=(n_blk + n_own,),
        in_specs=[
            pl.BlockSpec((1, n_own, tok), lambda s: (blk(s), 0, 0)),
            pl.BlockSpec((1, tok, d_model), lambda s: (blk(s), 0, 0)),
            pl.BlockSpec((1, d_model, ff), lambda s: (exp(s), 0, 0)),
            pl.BlockSpec((1, d_model, ff), lambda s: (exp(s), 0, 0)),
        ],
        out_specs=pl.BlockSpec((1, m, ff), lambda s: (exp(s), 0, 0)),
        out_shape=jax.ShapeDtypeStruct((n_own, m, ff), BF16),
        scratch_shapes=[pltpu.VMEM((n_own, m, d_model), BF16)],
        compiler_params=pltpu.CompilerParams(vmem_limit_bytes=48 << 20),
        cost_estimate=pl.CostEstimate(flops=flops, bytes_accessed=2 * (n_blk * tok * d_model + 2 * n_own * d_model * ff), transcendentals=n_own * m * ff),
    )(slot_own, x_all, wg, wu)


def gate_parts(g):
    hi = g.astype(BF16)
    rest = g - hi.astype(F32)
    mid = rest.astype(BF16)
    return hi, mid, (rest - mid.astype(F32)).astype(BF16)


def combine_kernel(n_down, n_blk, cap, n_loc, table_ref, h_ref, wd_ref, out_ref, o_rows):
    step = pl.program_id(0)
    per = h_ref.shape[0]
    cols = wd_ref.shape[2]

    @pl.when(step < n_down)
    def _():
        for i in range(per):
            o = jnp.dot(h_ref[i], wd_ref[i], preferred_element_type=F32).astype(BF16)
            at = pl.ds(pl.multiple_of((step * per + i) * cap, cap), cap)
            o_rows[:, at, :] = o.reshape(n_blk, cap, cols)

    @pl.when(step >= n_down)
    def _():
        table = table_ref[0]
        o = o_rows[step - n_down]
        tok = table.shape[0]
        lane = lax.broadcasted_iota(jnp.int32, (tok, LANES), 1)
        cid = (lane % cap).astype(F32)
        gs = []
        for k in range(n_loc * cap // LANES):
            src = lane // cap + k * (LANES // cap)
            slot = jnp.take_along_axis(table, src, axis=1)
            gate = jnp.take_along_axis(table, src + n_loc, axis=1)
            gs.append(gate_parts(jnp.where(slot == cid, gate, 0.0)))
        acc = None
        for part in range(3):
            mat = jnp.concatenate([g[part] for g in gs], axis=1)
            term = jnp.dot(mat, o, preferred_element_type=F32)
            acc = term if acc is None else acc + term
        out_ref[0] = acc


def combine_chunk(y, n_data, cap, table, h_all, wd):
    n_loc, m, ff = h_all.shape
    cols = wd.shape[2]
    tok = table.shape[1]
    n_blk = m // cap
    per = 4
    n_down = n_loc // per
    down = lambda s: jnp.minimum(s, n_down - 1)
    blk = lambda s: jnp.maximum(s - n_down, 0)
    flops = 2 * n_loc * m * ff * cols + 6 * n_blk * tok * n_loc * cap * cols
    return pl.pallas_call(
        functools.partial(combine_kernel, n_down, n_blk, cap, n_loc),
        grid=(n_down + n_blk,),
        in_specs=[
            pl.BlockSpec((1, tok, LANES), lambda s: (blk(s) * n_data + y, 0, 0)),
            pl.BlockSpec((per, m, ff), lambda s: (down(s), 0, 0)),
            pl.BlockSpec((per, ff, cols), lambda s: (down(s), 0, 0)),
        ],
        out_specs=pl.BlockSpec((1, tok, cols), lambda s: (blk(s), 0, 0)),
        out_shape=jax.ShapeDtypeStruct((n_blk, tok, cols), F32),
        scratch_shapes=[pltpu.VMEM((n_blk, n_loc * cap, cols), BF16)],
        compiler_params=pltpu.CompilerParams(vmem_limit_bytes=48 << 20),
        cost_estimate=pl.CostEstimate(flops=flops, bytes_accessed=2 * n_loc * (m * ff + ff * cols) + 4 * n_blk * tok * cols, transcendentals=0),
    )(table, h_all, wd)


def routing_tables(idx_all, gate_all, first_loc, n_loc, first_own, n_own, cap):
    tok = idx_all.shape[1]
    before = jnp.tril(jnp.ones((tok, tok), BF16), -1)

    def chosen_of(first, count):
        ids = (first + jnp.arange(count)).astype(F32)
        hit = idx_all[:, :, :, None] == ids
        return hit, jnp.any(hit, axis=2)

    hit, chosen = chosen_of(first_loc, n_loc)
    gate = jnp.sum(jnp.where(hit, gate_all[:, :, :, None], 0.0), axis=2)
    rank = jnp.einsum("st,bte->bse", before, chosen.astype(BF16), preferred_element_type=F32)
    slot = jnp.where(chosen & (rank < cap), rank, -1.0)
    fill = jnp.zeros(slot.shape[:2] + (LANES - 2 * n_loc,), F32)
    table = jnp.concatenate([slot, gate, fill], axis=2)
    own = lax.dynamic_slice_in_dim(slot, first_own - first_loc, n_own, axis=2)
    slot_own = jnp.swapaxes(own, 1, 2).astype(jnp.int32)
    return table, slot_own


def solution(mesh):
    exp_n = mesh.shape["expert"]
    n_data = mesh.shape["data"]
    tok_spec = P(("rep", "expert", "data"), None)
    group_axes = ("expert", "data")

    def device_fn(x_loc, idx_loc, gate_loc, wg_loc, wu_loc, wd_loc, wsg_loc, wsu_loc, wsd_loc):
        tok_count, d_model = x_loc.shape
        top = idx_loc.shape[1]
        n_loc, _, ff = wg_loc.shape
        cols = wd_loc.shape[2]
        n_own = n_loc // n_data
        cap = capacity_of(tok_count, top, n_loc * exp_n)
        pos = lax.axis_index("expert")
        dat = lax.axis_index("data")
        n_src = exp_n * n_data

        routing = jnp.concatenate([idx_loc.astype(F32), gate_loc], axis=1)
        routing = lax.all_gather(routing, group_axes, axis=0)
        x_all = lax.all_gather(x_loc, group_axes, axis=0)
        wg = lax.all_to_all(wg_loc, "data", 0, 1, tiled=True)
        wu = lax.all_to_all(wu_loc, "data", 0, 1, tiled=True)

        ws_loc = jnp.concatenate([wsg_loc, wsu_loc, wsd_loc.T], axis=1)
        ws = lax.all_gather(ws_loc, group_axes, axis=0, tiled=True)
        ffs = wsg_loc.shape[1]
        pre = jnp.dot(x_loc, ws[:, : 2 * ffs], preferred_element_type=F32)
        hs = (jax.nn.silu(pre[:, :ffs]) * pre[:, ffs:]).astype(BF16)
        hs_all = lax.all_gather(hs, "data", axis=0)
        wsd = lax.dynamic_slice_in_dim(ws[:, 2 * ffs :], dat * cols, cols, axis=0)

        table, slot_own = routing_tables(routing[:, :, :top], routing[:, :, top:], pos * n_loc, n_loc, pos * n_loc + dat * n_own, n_own, cap)

        sums = []
        for y in range(n_data):
            h = hidden_chunk(y, n_data, cap, slot_own, x_all, wg, wu)
            h_all = lax.all_gather(h, "data", axis=0, tiled=True)
            part = combine_chunk(y, n_data, cap, table, h_all, wd_loc)
            sums.append(lax.psum_scatter(part, "expert", scatter_dimension=0, tiled=True))

        routed = jnp.concatenate(sums, axis=0)
        shared = jnp.einsum("ytf,cf->ytc", hs_all, wsd, preferred_element_type=F32)
        mine = lax.dynamic_slice(x_all, (pos * n_data, 0, dat * cols), (n_data, tok_count, cols))
        out = (mine.astype(F32) + shared + routed).astype(BF16)
        return lax.all_to_all(out, "data", 0, 2, tiled=True).reshape(tok_count, d_model)

    in_specs = (tok_spec, tok_spec, tok_spec, P("expert", "data", None), P("expert", "data", None), P("expert", None, "data"), P(group_axes, None), P(group_axes, None), P(None, group_axes))
    return jax.shard_map(device_fn, mesh=mesh, in_specs=in_specs, out_specs=tok_spec, check_vma=False)
```

```python
import functools

import jax
import jax.numpy as jnp
from jax import lax
from jax.experimental import pallas as pl
from jax.experimental.pallas import tpu as pltpu
from jax.sharding import PartitionSpec as P


CAP_NUM = 5
CAP_DEN = 4
LANES = 128
BF16 = jnp.bfloat16
F32 = jnp.float32


def capacity_of(tok_count, top_count, n_exp):
    return max(8, ((CAP_NUM * top_count * tok_count) // (CAP_DEN * n_exp) + 7) // 8 * 8)


def hidden_kernel(n_blk, cap, slot_ref, x_ref, wg_ref, wu_ref, h_ref, rows):
    step = pl.program_id(0)
    n_own, tok = slot_ref.shape[1:]

    @pl.when(step < n_blk)
    def _():
        slot = slot_ref[0]
        cid = lax.broadcasted_iota(jnp.int32, (cap, tok), 0)
        pick = jnp.concatenate([jnp.where(slot[e : e + 1, :] == cid, 1.0, 0.0).astype(BF16) for e in range(n_own)], axis=0)
        got = jnp.dot(pick, x_ref[0], preferred_element_type=F32).astype(BF16)
        at = pl.ds(pl.multiple_of(step * cap, cap), cap)
        for e in range(n_own):
            rows[e, at, :] = got[e * cap : (e + 1) * cap, :]

    @pl.when(step >= n_blk)
    def _():
        tok_rows = rows[step - n_blk]
        d_model = tok_rows.shape[1]
        gate_pre = jnp.dot(tok_rows, wg_ref[...].reshape(d_model, -1), preferred_element_type=F32)
        up_pre = jnp.dot(tok_rows, wu_ref[...].reshape(d_model, -1), preferred_element_type=F32)
        h_ref[0] = (jax.nn.silu(gate_pre) * up_pre).astype(BF16)


def hidden_chunk(y, n_data, cap, slot_own, x_chunk, wg, wu):
    _, n_own, depth, ff = wg.shape
    n_blk, tok, d_model = x_chunk.shape
    m = n_blk * cap
    blk = lambda s: jnp.minimum(s, n_blk - 1)
    exp = lambda s: jnp.maximum(s - n_blk, 0)
    flops = 2 * n_blk * n_own * cap * tok * d_model + 4 * m * n_own * d_model * ff
    return pl.pallas_call(
        functools.partial(hidden_kernel, n_blk, cap),
        grid=(n_blk + n_own,),
        in_specs=[
            pl.BlockSpec((1, n_own, tok), lambda s: (blk(s) * n_data + y, 0, 0)),
            pl.BlockSpec((1, tok, d_model), lambda s: (blk(s), 0, 0)),
            pl.BlockSpec((n_data, 1, depth, ff), lambda s: (0, exp(s), 0, 0)),
            pl.BlockSpec((n_data, 1, depth, ff), lambda s: (0, exp(s), 0, 0)),
        ],
        out_specs=pl.BlockSpec((1, m, ff), lambda s: (exp(s), 0, 0)),
        out_shape=jax.ShapeDtypeStruct((n_own, m, ff), BF16),
        scratch_shapes=[pltpu.VMEM((n_own, m, d_model), BF16)],
        compiler_params=pltpu.CompilerParams(vmem_limit_bytes=48 << 20),
        cost_estimate=pl.CostEstimate(flops=flops, bytes_accessed=2 * (n_blk * tok * d_model + 2 * n_own * d_model * ff), transcendentals=n_own * m * ff),
    )(slot_own, x_chunk, wg, wu)


def gate_parts(g):
    hi = g.astype(BF16)
    rest = g - hi.astype(F32)
    mid = rest.astype(BF16)
    return hi, mid, (rest - mid.astype(F32)).astype(BF16)


def combine_kernel(n_blk, cap, n_loc, order_ref, table_ref, own_ref, right_ref, far_a_ref, far_b_ref, left_ref, wd_ref, out_ref, o_rows):
    step = pl.program_id(0)
    per = own_ref.shape[0]
    n_down = n_loc // per
    cols = wd_ref.shape[1]

    def down(h_ref):
        for i in range(per):
            o = lax.dot_general(h_ref[i], wd_ref[i], (((1,), (1,)), ((), ())), preferred_element_type=F32).astype(BF16)
            at = pl.ds(pl.multiple_of((step * per + i) * cap, cap), cap)
            o_rows[:, at, :] = o.reshape(n_blk, cap, cols)

    half = n_down // 8
    groups = ((0, 2, own_ref), (2, 4, right_ref), (4, 5, far_a_ref), (5, 6, far_b_ref), (6, 8, left_ref))
    for first, last, h_ref in groups:
        pl.when((step >= first * half) & (step < last * half))(functools.partial(down, h_ref))

    @pl.when(step >= n_down)
    def _():
        table = table_ref[0]
        o = o_rows[step - n_down]
        tok = table.shape[0]
        lane = lax.broadcasted_iota(jnp.int32, (tok, LANES), 1)
        cid = (lane % cap).astype(F32)
        gs = []
        for k in range(n_loc * cap // LANES):
            src = lane // cap + k * (LANES // cap)
            slot = jnp.take_along_axis(table, src, axis=1)
            gate = jnp.take_along_axis(table, src + n_loc, axis=1)
            gs.append(gate_parts(jnp.where(slot == cid, gate, 0.0)))
        acc = None
        for part in range(3):
            mat = jnp.concatenate([g[part] for g in gs], axis=1)
            term = jnp.dot(mat, o, preferred_element_type=F32)
            acc = term if acc is None else acc + term
        out_ref[0] = acc


def combine_chunk(y, n_data, cap, order, table, pieces, wd_t):
    n_loc, cols, ff = wd_t.shape
    m = pieces[0].shape[1]
    tok = table.shape[1]
    n_blk = m // cap
    n_down = order.shape[0]
    per = n_loc // n_down
    half = n_down // 8
    down = lambda s: jnp.minimum(s, n_down - 1)
    blk = lambda s: jnp.maximum(s - n_down, 0)

    def piece_spec(first, piece):
        last = piece.shape[0] // per - 1
        return pl.BlockSpec((per, m, ff), lambda s, o: (jnp.clip(s - first * half, 0, last), 0, 0))

    flops = 2 * n_loc * m * ff * cols + 6 * n_blk * tok * n_loc * cap * cols
    return pl.pallas_call(
        functools.partial(combine_kernel, n_blk, cap, n_loc),
        grid_spec=pltpu.PrefetchScalarGridSpec(
            num_scalar_prefetch=1,
            grid=(n_down + n_blk,),
            in_specs=[pl.BlockSpec((1, tok, LANES), lambda s, o: (blk(s) * n_data + y, 0, 0))]
            + [piece_spec(first, piece) for first, piece in zip((0, 2, 4, 5, 6), pieces)]
            + [pl.BlockSpec((per, cols, ff), lambda s, o: (o[down(s)], 0, 0))],
            out_specs=pl.BlockSpec((1, tok, cols), lambda s, o: (blk(s), 0, 0)),
            scratch_shapes=[pltpu.VMEM((n_blk, n_loc * cap, cols), BF16)],
        ),
        out_shape=jax.ShapeDtypeStruct((n_blk, tok, cols), F32),
        compiler_params=pltpu.CompilerParams(vmem_limit_bytes=48 << 20),
        cost_estimate=pl.CostEstimate(flops=flops, bytes_accessed=2 * n_loc * (m * ff + ff * cols) + 4 * n_blk * tok * cols, transcendentals=0),
    )(order, table, *pieces, wd_t)


def ring_gather(h, n_data):
    up = [(i, (i + 1) % n_data) for i in range(n_data)]
    down = [(i, (i - 1) % n_data) for i in range(n_data)]
    half = h.shape[0] // 2
    right = lax.ppermute(h, "data", down)
    left = lax.ppermute(h, "data", up)
    far_a = lax.ppermute(left[:half], "data", up)
    far_b = lax.ppermute(right[half:], "data", down)
    return h, right, far_a, far_b, left


def routing_tables(idx_all, gate_all, ids, n_own, cap):
    tok = idx_all.shape[1]
    before = jnp.tril(jnp.ones((tok, tok), BF16), -1)
    hit = idx_all[:, :, :, None] == ids.astype(F32)
    chosen = jnp.any(hit, axis=2)
    gate = jnp.sum(jnp.where(hit, gate_all[:, :, :, None], 0.0), axis=2)
    rank = jnp.einsum("st,bte->bse", before, chosen.astype(BF16), preferred_element_type=F32)
    slot = jnp.where(chosen & (rank < cap), rank, -1.0)
    fill = jnp.zeros(slot.shape[:2] + (LANES - 2 * ids.shape[0],), F32)
    table = jnp.concatenate([slot, gate, fill], axis=2)
    slot_own = jnp.swapaxes(slot[:, :, :n_own], 1, 2).astype(jnp.int32)
    return table, slot_own


def solution(mesh):
    exp_n = mesh.shape["expert"]
    n_data = mesh.shape["data"]
    tok_spec = P(("rep", "expert", "data"), None)
    group_axes = ("expert", "data")

    def device_fn(x_loc, idx_loc, gate_loc, wg_loc, wu_loc, wd_loc, wsg_loc, wsu_loc, wsd_loc):
        tok_count, d_model = x_loc.shape
        top = idx_loc.shape[1]
        n_loc, _, ff = wg_loc.shape
        cols = wd_loc.shape[2]
        n_own = n_loc // n_data
        cap = capacity_of(tok_count, top, n_loc * exp_n)
        pos = lax.axis_index("expert")
        dat = lax.axis_index("data")

        def gather(value, axes, tiled=False):
            return lax.all_gather(value, axes, axis=0, tiled=tiled)

        def exchange(w):
            return lax.all_to_all(w.reshape(n_data, n_own, -1, ff), "data", 0, 0)

        x_pos = gather(x_loc, "data")
        idx_all = gather(idx_loc.astype(F32), group_axes)
        gate_all = gather(gate_loc, group_axes)
        chunks = [gather(x_pos[y], "expert") for y in range(n_data)]
        wg = exchange(wg_loc)
        wu = exchange(wu_loc)

        ring = (dat + jnp.arange(n_data)) % n_data
        ids = pos * n_loc + (ring[:, None] * n_own + jnp.arange(n_own)).reshape(-1)
        order = (ring[:, None] * 2 + jnp.arange(2)).reshape(-1).astype(jnp.int32)
        table, slot_own = routing_tables(idx_all, gate_all, ids, n_own, cap)

        ws = gather(jnp.concatenate([wsg_loc, wsu_loc, wsd_loc.T], axis=1), group_axes, tiled=True)
        ffs = wsg_loc.shape[1]
        pre = jnp.dot(x_loc, ws[:, : 2 * ffs], preferred_element_type=F32)
        hs = (jax.nn.silu(pre[:, :ffs]) * pre[:, ffs:]).astype(BF16)
        hs_all = gather(hs, "data")
        wsd = lax.dynamic_slice_in_dim(ws[:, 2 * ffs :], dat * cols, cols, axis=0)

        wd_t = jnp.swapaxes(wd_loc, 1, 2)
        sums = []
        for y in range(n_data):
            h = hidden_chunk(y, n_data, cap, slot_own, chunks[y], wg, wu)
            pieces = ring_gather(h, n_data)
            part = combine_chunk(y, n_data, cap, order, table, pieces, wd_t)
            sums.append(lax.psum_scatter(part, "expert", scatter_dimension=0, tiled=True))

        routed = jnp.concatenate(sums, axis=0)
        shared = jnp.einsum("ytf,cf->ytc", hs_all, wsd, preferred_element_type=F32)
        mine = lax.dynamic_slice_in_dim(x_pos, dat * cols, cols, axis=2)
        out = (mine.astype(F32) + shared + routed).astype(BF16)
        return lax.all_to_all(out, "data", 0, 2, tiled=True).reshape(tok_count, d_model)

    in_specs = (tok_spec, tok_spec, tok_spec, P("expert", "data", None), P("expert", "data", None), P("expert", None, "data"), P(group_axes, None), P(group_axes, None), P(None, group_axes))
    return jax.shard_map(device_fn, mesh=mesh, in_specs=in_specs, out_specs=tok_spec, check_vma=False)
```

```python
import functools

import jax
import jax.numpy as jnp
from jax import lax
from jax.experimental import pallas as pl
from jax.experimental.pallas import tpu as pltpu
from jax.sharding import PartitionSpec as P


CAP_NUM = 5
CAP_DEN = 4
LANES = 128
BF16 = jnp.bfloat16
F32 = jnp.float32


def capacity_of(tok_count, top_count, n_exp):
    return max(8, ((CAP_NUM * top_count * tok_count) // (CAP_DEN * n_exp) + 7) // 8 * 8)


def hidden_kernel(n_blk, cap, slot_ref, x_ref, wg_ref, wu_ref, h_ref, rows):
    step = pl.program_id(0)
    n_own, tok = slot_ref.shape[1:]

    @pl.when(step < n_blk)
    def _():
        slot = slot_ref[0]
        cid = lax.broadcasted_iota(jnp.int32, (cap, tok), 0)
        pick = jnp.concatenate([jnp.where(slot[e : e + 1, :] == cid, 1.0, 0.0).astype(BF16) for e in range(n_own)], axis=0)
        got = jnp.dot(pick, x_ref[0], preferred_element_type=F32).astype(BF16)
        at = pl.ds(pl.multiple_of(step * cap, cap), cap)
        for e in range(n_own):
            rows[e, at, :] = got[e * cap : (e + 1) * cap, :]

    @pl.when(step >= n_blk)
    def _():
        tok_rows = rows[step - n_blk]
        d_model = tok_rows.shape[1]
        gate_pre = jnp.dot(tok_rows, wg_ref[...].reshape(d_model, -1), preferred_element_type=F32)
        up_pre = jnp.dot(tok_rows, wu_ref[...].reshape(d_model, -1), preferred_element_type=F32)
        h_ref[0] = (jax.nn.silu(gate_pre) * up_pre).astype(BF16)


def hidden_chunk(y, n_data, cap, slot_own, x_chunk, wg, wu):
    _, n_own, depth, ff = wg.shape
    n_blk, tok, d_model = x_chunk.shape
    m = n_blk * cap
    blk = lambda s: jnp.minimum(s, n_blk - 1)
    exp = lambda s: jnp.maximum(s - n_blk, 0)
    flops = 2 * n_blk * n_own * cap * tok * d_model + 4 * m * n_own * d_model * ff
    return pl.pallas_call(
        functools.partial(hidden_kernel, n_blk, cap),
        grid=(n_blk + n_own,),
        in_specs=[
            pl.BlockSpec((1, n_own, tok), lambda s: (blk(s) * n_data + y, 0, 0)),
            pl.BlockSpec((1, tok, d_model), lambda s: (blk(s), 0, 0)),
            pl.BlockSpec((n_data, 1, depth, ff), lambda s: (0, exp(s), 0, 0)),
            pl.BlockSpec((n_data, 1, depth, ff), lambda s: (0, exp(s), 0, 0)),
        ],
        out_specs=pl.BlockSpec((1, m, ff), lambda s: (exp(s), 0, 0)),
        out_shape=jax.ShapeDtypeStruct((n_own, m, ff), BF16),
        scratch_shapes=[pltpu.VMEM((n_own, m, d_model), BF16)],
        compiler_params=pltpu.CompilerParams(vmem_limit_bytes=48 << 20),
        cost_estimate=pl.CostEstimate(flops=flops, bytes_accessed=2 * (n_blk * tok * d_model + 2 * n_own * d_model * ff), transcendentals=n_own * m * ff),
    )(slot_own, x_chunk, wg, wu)


def pick_kernel(cap, slot_ref, x_ref, rows_ref):
    n_own, tok = slot_ref.shape[1:]
    slot = slot_ref[0]
    cid = lax.broadcasted_iota(jnp.int32, (cap, tok), 0)
    pick = jnp.concatenate([jnp.where(slot[e : e + 1, :] == cid, 1.0, 0.0).astype(BF16) for e in range(n_own)], axis=0)
    got = jnp.dot(pick, x_ref[0], preferred_element_type=F32).astype(BF16)
    rows_ref[...] = got.reshape(rows_ref.shape)


def pick_chunk(y, n_data, cap, slot_own, x_chunk):
    n_own = slot_own.shape[1]
    n_blk, tok, d_model = x_chunk.shape
    return pl.pallas_call(
        functools.partial(pick_kernel, cap),
        grid=(n_blk,),
        in_specs=[
            pl.BlockSpec((1, n_own, tok), lambda s: (s * n_data + y, 0, 0)),
            pl.BlockSpec((1, tok, d_model), lambda s: (s, 0, 0)),
        ],
        out_specs=pl.BlockSpec((n_own, cap, d_model), lambda s: (0, s, 0)),
        out_shape=jax.ShapeDtypeStruct((n_own, n_blk * cap, d_model), BF16),
        compiler_params=pltpu.CompilerParams(vmem_limit_bytes=32 << 20),
        cost_estimate=pl.CostEstimate(flops=2 * n_blk * n_own * cap * tok * d_model, bytes_accessed=2 * n_blk * (tok + n_own * cap) * d_model, transcendentals=0),
    )(slot_own, x_chunk)


def expert_kernel(rows_ref, wg_ref, wu_ref, h_ref):
    tok_rows = rows_ref[0]
    d_model = tok_rows.shape[1]
    gate_pre = jnp.dot(tok_rows, wg_ref[...].reshape(d_model, -1), preferred_element_type=F32)
    up_pre = jnp.dot(tok_rows, wu_ref[...].reshape(d_model, -1), preferred_element_type=F32)
    h_ref[0] = (jax.nn.silu(gate_pre) * up_pre).astype(BF16)


def expert_chunk(rows, wg, wu):
    n_data, n_own, depth, ff = wg.shape
    _, m, d_model = rows.shape
    return pl.pallas_call(
        expert_kernel,
        grid=(n_own,),
        in_specs=[
            pl.BlockSpec((1, m, d_model), lambda s: (s, 0, 0)),
            pl.BlockSpec((n_data, 1, depth, ff), lambda s: (0, s, 0, 0)),
            pl.BlockSpec((n_data, 1, depth, ff), lambda s: (0, s, 0, 0)),
        ],
        out_specs=pl.BlockSpec((1, m, ff), lambda s: (s, 0, 0)),
        out_shape=jax.ShapeDtypeStruct((n_own, m, ff), BF16),
        compiler_params=pltpu.CompilerParams(vmem_limit_bytes=32 << 20),
        cost_estimate=pl.CostEstimate(flops=4 * m * n_own * d_model * ff, bytes_accessed=2 * n_own * d_model * (m + 2 * ff), transcendentals=n_own * m * ff),
    )(rows, wg, wu)


def gate_parts(g):
    hi = g.astype(BF16)
    rest = g - hi.astype(F32)
    mid = rest.astype(BF16)
    return hi, mid, (rest - mid.astype(F32)).astype(BF16)


def combine_kernel(n_blk, cap, n_loc, order_ref, table_ref, own_ref, right_ref, far_a_ref, far_b_ref, left_ref, wd_ref, out_ref, o_rows):
    step = pl.program_id(0)
    per = own_ref.shape[0]
    n_down = n_loc // per
    cols = wd_ref.shape[1]

    def down(h_ref):
        for i in range(per):
            o = lax.dot_general(h_ref[i], wd_ref[i], (((1,), (1,)), ((), ())), preferred_element_type=F32).astype(BF16)
            at = pl.ds(pl.multiple_of((step * per + i) * cap, cap), cap)
            o_rows[:, at, :] = o.reshape(n_blk, cap, cols)

    half = n_down // 8
    groups = ((0, 2, own_ref), (2, 4, right_ref), (4, 5, far_a_ref), (5, 6, far_b_ref), (6, 8, left_ref))
    for first, last, h_ref in groups:
        pl.when((step >= first * half) & (step < last * half))(functools.partial(down, h_ref))

    @pl.when(step >= n_down)
    def _():
        table = table_ref[0]
        o = o_rows[step - n_down]
        tok = table.shape[0]
        lane = lax.broadcasted_iota(jnp.int32, (tok, LANES), 1)
        cid = (lane % cap).astype(F32)
        gs = []
        for k in range(n_loc * cap // LANES):
            src = lane // cap + k * (LANES // cap)
            slot = jnp.take_along_axis(table, src, axis=1)
            gate = jnp.take_along_axis(table, src + n_loc, axis=1)
            gs.append(gate_parts(jnp.where(slot == cid, gate, 0.0)))
        acc = None
        for part in range(3):
            mat = jnp.concatenate([g[part] for g in gs], axis=1)
            term = jnp.dot(mat, o, preferred_element_type=F32)
            acc = term if acc is None else acc + term
        out_ref[0] = acc


def combine_chunk(y, n_data, cap, order, table, pieces, wd_t):
    n_loc, cols, ff = wd_t.shape
    m = pieces[0].shape[1]
    tok = table.shape[1]
    n_blk = m // cap
    n_down = order.shape[0]
    per = n_loc // n_down
    half = n_down // 8
    down = lambda s: jnp.minimum(s, n_down - 1)
    blk = lambda s: jnp.maximum(s - n_down, 0)

    def piece_spec(first, piece):
        last = piece.shape[0] // per - 1
        return pl.BlockSpec((per, m, ff), lambda s, o: (jnp.clip(s - first * half, 0, last), 0, 0))

    flops = 2 * n_loc * m * ff * cols + 6 * n_blk * tok * n_loc * cap * cols
    return pl.pallas_call(
        functools.partial(combine_kernel, n_blk, cap, n_loc),
        grid_spec=pltpu.PrefetchScalarGridSpec(
            num_scalar_prefetch=1,
            grid=(n_down + n_blk,),
            in_specs=[pl.BlockSpec((1, tok, LANES), lambda s, o: (blk(s) * n_data + y, 0, 0))]
            + [piece_spec(first, piece) for first, piece in zip((0, 2, 4, 5, 6), pieces)]
            + [pl.BlockSpec((per, cols, ff), lambda s, o: (o[down(s)], 0, 0))],
            out_specs=pl.BlockSpec((1, tok, cols), lambda s, o: (blk(s), 0, 0)),
            scratch_shapes=[pltpu.VMEM((n_blk, n_loc * cap, cols), BF16)],
        ),
        out_shape=jax.ShapeDtypeStruct((n_blk, tok, cols), F32),
        compiler_params=pltpu.CompilerParams(vmem_limit_bytes=48 << 20),
        cost_estimate=pl.CostEstimate(flops=flops, bytes_accessed=2 * n_loc * (m * ff + ff * cols) + 4 * n_blk * tok * cols, transcendentals=0),
    )(order, table, *pieces, wd_t)


def ring_gather(h, n_data):
    up = [(i, (i + 1) % n_data) for i in range(n_data)]
    down = [(i, (i - 1) % n_data) for i in range(n_data)]
    half = h.shape[0] // 2
    right = lax.ppermute(h, "data", down)
    left = lax.ppermute(h, "data", up)
    far_a = lax.ppermute(left[:half], "data", up)
    far_b = lax.ppermute(right[half:], "data", down)
    return h, right, far_a, far_b, left


def routing_tables(idx_all, gate_all, ids, n_own, cap):
    tok = idx_all.shape[1]
    before = jnp.tril(jnp.ones((tok, tok), BF16), -1)
    hit = idx_all[:, :, :, None] == ids.astype(F32)
    chosen = jnp.any(hit, axis=2)
    gate = jnp.sum(jnp.where(hit, gate_all[:, :, :, None], 0.0), axis=2)
    rank = jnp.einsum("st,bte->bse", before, chosen.astype(BF16), preferred_element_type=F32)
    slot = jnp.where(chosen & (rank < cap), rank, -1.0)
    fill = jnp.zeros(slot.shape[:2] + (LANES - 2 * ids.shape[0],), F32)
    table = jnp.concatenate([slot, gate, fill], axis=2)
    slot_own = jnp.swapaxes(slot[:, :, :n_own], 1, 2).astype(jnp.int32)
    return table, slot_own


def solution(mesh):
    exp_n = mesh.shape["expert"]
    n_data = mesh.shape["data"]
    tok_spec = P(("rep", "expert", "data"), None)
    group_axes = ("expert", "data")

    def device_fn(x_loc, idx_loc, gate_loc, wg_loc, wu_loc, wd_loc, wsg_loc, wsu_loc, wsd_loc):
        tok_count, d_model = x_loc.shape
        top = idx_loc.shape[1]
        n_loc, _, ff = wg_loc.shape
        cols = wd_loc.shape[2]
        n_own = n_loc // n_data
        cap = capacity_of(tok_count, top, n_loc * exp_n)
        pos = lax.axis_index("expert")
        dat = lax.axis_index("data")

        def gather(value, axes, tiled=False):
            return lax.all_gather(value, axes, axis=0, tiled=tiled)

        def exchange(w):
            return lax.all_to_all(w.reshape(n_data, n_own, -1, ff), "data", 0, 0)

        x_pos = gather(x_loc, "data")
        idx_all = gather(idx_loc.astype(F32), group_axes)
        gate_all = gather(gate_loc, group_axes)
        chunks = [gather(x_pos[y], "expert") for y in range(n_data)]
        wg = exchange(wg_loc)
        wu = exchange(wu_loc)

        ring = (dat + jnp.arange(n_data)) % n_data
        ids = pos * n_loc + (ring[:, None] * n_own + jnp.arange(n_own)).reshape(-1)
        order = (ring[:, None] * 2 + jnp.arange(2)).reshape(-1).astype(jnp.int32)
        table, slot_own = routing_tables(idx_all, gate_all, ids, n_own, cap)

        ws = gather(jnp.concatenate([wsg_loc, wsu_loc, wsd_loc.T], axis=1), group_axes, tiled=True)
        ffs = wsg_loc.shape[1]
        pre = jnp.dot(x_loc, ws[:, : 2 * ffs], preferred_element_type=F32)
        hs = (jax.nn.silu(pre[:, :ffs]) * pre[:, ffs:]).astype(BF16)
        hs, hs_right, hs_a, hs_b, hs_left = ring_gather(hs, n_data)
        hs_ring = [hs, hs_right, jnp.concatenate([hs_a, hs_b], axis=0), hs_left]
        hs_all = lax.dynamic_slice_in_dim(jnp.stack(hs_ring + hs_ring), (n_data - dat) % n_data, n_data, axis=0)
        wsd = lax.dynamic_slice_in_dim(ws[:, 2 * ffs :], dat * cols, cols, axis=0)

        wd_t = jnp.swapaxes(wd_loc, 1, 2)
        rows = pick_chunk(0, n_data, cap, slot_own, chunks[0])
        sums = []
        for y in range(n_data):
            h = expert_chunk(rows, wg, wu) if y == 0 else hidden_chunk(y, n_data, cap, slot_own, chunks[y], wg, wu)
            pieces = ring_gather(h, n_data)
            part = combine_chunk(y, n_data, cap, order, table, pieces, wd_t)
            sums.append(lax.psum_scatter(part, "expert", scatter_dimension=0, tiled=True))

        routed = jnp.concatenate(sums, axis=0)
        shared = jnp.einsum("ytf,cf->ytc", hs_all, wsd, preferred_element_type=F32)
        mine = lax.dynamic_slice_in_dim(x_pos, dat * cols, cols, axis=2)
        out = (mine.astype(F32) + shared + routed).astype(BF16)
        return lax.all_to_all(out, "data", 0, 2, tiled=True).reshape(tok_count, d_model)

    in_specs = (tok_spec, tok_spec, tok_spec, P("expert", "data", None), P("expert", "data", None), P("expert", None, "data"), P(group_axes, None), P(group_axes, None), P(None, group_axes))
    return jax.shard_map(device_fn, mesh=mesh, in_specs=in_specs, out_specs=tok_spec, check_vma=False)
```
